32 devices in a mesh: grp: 4 (over x, core), mem: 8 (over z, y).
Axes of the slice: x: 2, y: 2, z: 4, core: 2. Of those that a mesh axis runs over, the one named last changes fastest.
Arguments:
- images: bfloat16 [4, 2, 768, 16384], P('grp', None, None, 'mem'), may hold values from -6 to 6
- phantom: bfloat16 [4, 16384], P('grp', 'mem'), may hold values from -12 to 12
- inject_rows: int32 [4, 2, 64], P('grp'), may hold values from 0 to 767
- prior_blocks: int32 [4, 2, 768], P('grp'), may hold values from 0 to 127
- basis: bfloat16 [16384, 512], P('mem'), may hold values from -0.046875 to 0.046875
- refs: bfloat16 [512, 32768], P(None, 'mem'), may hold values from -24 to 24
Outputs:
- new_refs: float32 [512, 32768], P('grp', 'mem')
The draws below stay inside these ranges and needn't reach their ends.
Inputs may be any that keep to these rules, and one draw needn't show every extreme that they name: `inject_rows`: row numbers within a batch; repeats may occur. `prior_blocks`: orientation block numbers; block b holds orientations b * 256 to (b + 1) * 256 - 1.
All inputs are finite; a program needn't handle non-finite values.
Results may differ from the reference program's by a relative error of at most 0.0051.
Values sent between devices are 32-bit elements; how exact they have to be, the bound alone decides.
A program may use at most 128 MiB of HBM per device.

```python
import math
import jax
import jax.numpy as jnp
import numpy as np
from jax import lax

PARTICLES = 768
BATCHES = 2
PIXELS = 16384
EIGEN = 512
ORIENT = 32768
OBLOCK = 256
INJECTED = 64
GROUPS = 4


def draw_refs(key, part):
    keys = jax.random.split(jax.random.fold_in(key, 11), 1)
    return jnp.clip(jax.random.normal(keys[0], (EIGEN, ORIENT), jnp.float32) * 0.13, -0.8, 0.8).astype(jnp.bfloat16)


def place_ends(result, key, low, largest):
    index_at = [jax.random.randint(jax.random.fold_in(key, axis), (), 0, length) for axis, length in enumerate(result.shape)]
    widest = result.shape.index(max(result.shape))
    beside = index_at[:widest] + [(index_at[widest] + 1) % result.shape[widest]] + index_at[widest + 1:]
    return result.at[tuple(index_at)].set(low).at[tuple(beside)].set(largest)


def block_levels(stream_key, shape, cuts, least, high):
    level, own = 1.0, jax.random.fold_in(stream_key, 6)
    for position, blocks in cuts:
        steps = jnp.exp(jax.random.uniform(jax.random.fold_in(own, position), (blocks,), jnp.float32, least / len(cuts), high / len(cuts)))
        level = level * jnp.repeat(steps, shape[position] // blocks).reshape([-1 if axis == position else 1 for axis in range(len(shape))])
    return level


def cumulative_ranks(amount, slope):
    loads = [(1 << 20) // math.isqrt(rank ** slope) + 1 for rank in range(1, amount + 1)]
    deviation = 1 + sum(loads) // (1 << 30)
    return np.cumsum(np.array([max(1, weight // deviation) for weight in loads]))


def skewed_ids(key, shape, amount, slope):
    grid = cumulative_ranks(amount, slope)
    lot = jax.random.randint(jax.random.fold_in(key, 1), shape, 0, int(grid[amount - 1]))
    rank = jnp.searchsorted(jnp.asarray(grid, jnp.int32), lot, side="right")
    return jax.random.permutation(jax.random.fold_in(key, 2), amount)[rank].astype(jnp.int32)


def centred(stream_key, shape, scale, limit, pieces=(), kind=jnp.bfloat16):
    values = jax.random.normal(stream_key, shape, jnp.float32) * scale
    if len(pieces) > 0:
        values = block_levels(stream_key, shape, pieces, -0.22, 0.18) * values
    return jnp.clip(values, min=-limit, max=limit).astype(kind)


def setup_inputs(seed: int = 0) -> dict:
    key_of = jax.random.split(jax.random.key(seed), 7)
    images = centred(key_of[0], (GROUPS, BATCHES, PARTICLES, PIXELS), 1.0, 6.0, ((0, 4), (3, 8)))
    phantom = centred(key_of[1], (GROUPS, PIXELS), 2.0, 12.0, ((0, 4), (1, 8)))
    inject_rows = place_ends(jax.random.randint(key_of[2], (GROUPS, BATCHES, INJECTED), 0, PARTICLES), jax.random.fold_in(key_of[2], 1), 0, PARTICLES - 1).astype(jnp.int32)
    prior_blocks = place_ends(skewed_ids(key_of[3], (GROUPS, BATCHES, PARTICLES), ORIENT // OBLOCK, 2), jax.random.fold_in(key_of[3], 3), 0, (ORIENT // OBLOCK) - 1).astype(jnp.int32)
    basis = centred(key_of[4], (PIXELS, EIGEN), PIXELS ** -0.5, 0.046875, ((0, 8),))
    refs = draw_refs(jax.random.fold_in(key_of[6], 71), 0)
    return {"images": images, "phantom": phantom, "inject_rows": inject_rows, "prior_blocks": prior_blocks, "basis": basis, "refs": refs}


PRIOR_INCREMENT = 3.0


def reference(images, phantom, inject_rows, prior_blocks, basis, refs):
    positions = jnp.arange(PARTICLES, dtype=jnp.int32)
    orient_block = (jnp.arange(ORIENT, dtype=jnp.int32) // OBLOCK).astype(jnp.int32)

    def per_group(running, inputs):
        totals, masses = running
        group_images, group_phantom, group_rows, group_blocks = inputs
        phantom_coef = jnp.dot(group_phantom, basis, preferred_element_type=jnp.float32)
        for batch_index in range(BATCHES):
            chosen = jnp.any(group_rows[batch_index][:, None] == positions[None, :], axis=0).astype(jnp.float32)
            plain = jnp.dot(group_images[batch_index], basis, preferred_element_type=jnp.float32)
            basis_coefficients = (plain + chosen[:, None] * phantom_coef[None, :]).astype(jnp.bfloat16)
            match_score = (group_blocks[batch_index][:, None] == orient_block[None, :]).astype(jnp.float32)
            score_rows = jnp.dot(basis_coefficients, refs, preferred_element_type=jnp.float32) + PRIOR_INCREMENT * match_score
            row_top = jnp.max(score_rows, axis=1, keepdims=True)
            powers = jnp.exp(score_rows - row_top)
            weights = (powers / jnp.sum(powers, axis=1, keepdims=True)).astype(jnp.bfloat16)
            totals = totals + lax.dot_general(basis_coefficients, weights, (((0,), (0,)), ((), ())), preferred_element_type=jnp.float32)
            masses = masses + jnp.sum(weights.astype(jnp.float32), axis=0)
        return (totals, masses), None

    start = (jnp.zeros((EIGEN, ORIENT), jnp.float32), jnp.zeros((ORIENT,), jnp.float32))
    (totals, masses), unused = lax.scan(per_group, start, (images, phantom, inject_rows, prior_blocks))
    return (totals + refs.astype(jnp.float32)) / (masses[None, :] + 1.0)
```

```python
import functools

import jax
import jax.numpy as jnp
from jax import lax
from jax.experimental import pallas as pl
from jax.experimental.pallas import tpu as pltpu
from jax.sharding import PartitionSpec as P

OBLOCK = 256
PRIOR_INCREMENT = 3.0
MESH = pl.DeviceIdType.MESH
F32 = jnp.float32


def remote(src, dst, send_sem, recv_sem, device):
    return pltpu.make_async_remote_copy(
        src_ref=src, dst_ref=dst, send_sem=send_sem, recv_sem=recv_sem,
        device_id=device, device_id_type=MESH,
    )


def coeff_kernel(
    A, R, H,
    img, pha, chosen, basis, out,
    part0, part1, y0r, z0s, z0r, z1r, y1s, y1r, g0, g1,
    y0_ss, y0_rs, z0_ss, z0_rs, z1_ss, z1_rs, y1_ss, y1_rs,
    gz0_ss, gz0_rs, gy0_ss, gy0_rs, gy1_ss, gy1_rs, gz1_ss, gz1_rs,
):
    grp = lax.axis_index("grp")
    mem = lax.axis_index("mem")
    a, b = mem // 2, lax.rem(mem, 2)
    nb = 1 - b
    HR = R // 2
    ypeer = (grp, a * 2 + nb)

    def zpeer(k):
        return (grp, lax.rem(a + k, A) * 2 + b)

    barrier = pltpu.get_barrier_semaphore()
    pl.semaphore_signal(barrier, inc=1, device_id=ypeer, device_id_type=MESH)
    for k in range(1, A):
        pl.semaphore_signal(barrier, inc=1, device_id=zpeer(k), device_id_type=MESH)
    pl.semaphore_wait(barrier, A)

    phc = jnp.dot(pha[...], basis[...], preferred_element_type=F32)[0:1]

    def partial(k, bb, half):
        start = pl.multiple_of((lax.rem(a + k, A) * 2 + bb) * R, R)
        cols = slice(half * H, (half + 1) * H)
        plain = jnp.dot(img[pl.ds(start, R), :], basis[:, cols], preferred_element_type=F32)
        return plain + chosen[pl.ds(start, R), :] * phc[:, cols]

    ring = A == 4
    far = {0: 1, 1: A - 1}

    def zlink(k, h):
        return zpeer(far[h]) if ring and k == 2 else zpeer(k)

    near = [1, 3] if ring else list(range(1, A))
    pairs = [(k, h) for k in range(1, A) for h in range(2)]
    late = [(1, 0), (3, 1)] if ring else []
    y0 = [remote(part0.at[1, k], y0r.at[k], y0_ss.at[k], y0_rs.at[k], ypeer) for k in range(A)]
    z1 = {
        (k, h): remote(part1.at[k, h], z1r.at[k - 1, h], z1_ss.at[k - 1, h], z1_rs.at[k - 1, h], zlink(k, h))
        for k, h in pairs
    }
    order = [2, 1, 3, 0] if ring else [k % A for k in range(1, A + 1)]
    for k in order:
        part0[1, k] = partial(k, nb, 0)
        if k > 0:
            part1[k, 0] = partial(k, b, 1)
            part1[k, 1] = partial(k, nb, 1)
        y0[k].start()
        for h in range(2):
            if k > 0 and (k, h) not in late:
                z1[k, h].start()
    for k in order:
        part0[0, k] = partial(k, b, 0)
    part1[0, 0] = partial(0, b, 1)
    part1[0, 1] = partial(0, nb, 1)

    z0 = {
        (k, h): remote(z0s.at[k - 1, h], z0r.at[k - 1, h], z0_ss.at[k - 1, h], z0_rs.at[k - 1, h], zlink(k, h))
        for k, h in pairs
    }
    for k, h in late:
        z1[2, h].wait_recv()
        part1[k, h] = part1[k, h] + z1r[1, h]
        z1[k, h].start()
    for k in order[:-1]:
        y0[k].wait_recv()
        value = part0[0, k] + y0r[k]
        for h in range(2):
            z0s[k - 1, h] = value[h * HR:(h + 1) * HR]
            if (k, h) not in late:
                z0[k, h].start()
    for k, h in late:
        z0[2, h].wait_recv()
        z0s[k - 1, h] = z0s[k - 1, h] + z0r[1, h]
        z0[k, h].start()
    peer_sum = part1[0, 1]
    own_sum = part1[0, 0]
    for k in near:
        z1[k, 1].wait_recv()
        peer_sum = peer_sum + z1r[k - 1, 1]
    y1s[...] = peer_sum
    y1 = remote(y1s, y1r, y1_ss, y1_rs, ypeer)
    y1.start()
    for k in near:
        z1[k, 0].wait_recv()
        own_sum = own_sum + z1r[k - 1, 0]

    y0[0].wait_recv()
    mine0 = part0[0, 0] + y0r[0]
    for h in range(2):
        value = mine0[h * HR:(h + 1) * HR]
        for k in near:
            z0[k, h].wait_recv()
            value = value + z0r[k - 1, h]
        g0[0, 0, h] = value.astype(jnp.bfloat16).astype(F32)
    gz0 = {}
    gz1 = {}
    for k, h in pairs:
        source = far[h] if ring and k == 2 else 0
        gz0[k, h] = remote(
            g0.at[0, source, h], g0.at[0, k, h], gz0_ss.at[k - 1, h], gz0_rs.at[k - 1, h], zlink(k, h)
        )
        gz1[k, h] = remote(
            g1.at[source, h], g1.at[k, h], gz1_ss.at[k - 1, h], gz1_rs.at[k - 1, h], zlink(k, h)
        )
    gy0 = [remote(g0.at[0, k], g0.at[1, k], gy0_ss.at[k], gy0_rs.at[k], ypeer) for k in range(A)]
    for k, h in late + [(k, h) for k in near for h in range(2) if (k, h) not in late]:
        gz0[k, h].start()
    gy0[0].start()
    y1.wait_recv()
    g1[0, 0] = (own_sum + y1r[...]).astype(jnp.bfloat16).astype(F32)
    gy1 = remote(g1.at[0, 0], g1.at[0, 1], gy1_ss, gy1_rs, ypeer)
    gy1.start()
    for k in near:
        gz1[k, 0].start()
    for k, h in late:
        gz0[k, h].wait_recv()
        gz0[2, h].start()
    gy1.wait_recv()
    for k in near[::-1]:
        gz1[k, 1].start()
    for k in near:
        for h in range(2):
            if (k, h) not in late:
                gz0[k, h].wait_recv()
        gy0[k].start()
    for k, h in late:
        gz1[k, h].wait_recv()
        gz1[2, h].start()
    if ring:
        for h in range(2):
            gz0[2, h].wait_recv()
        gy0[2].start()

    def put(k, bb, half, value):
        start = pl.multiple_of((lax.rem(a - k + A, A) * 2 + bb) * R, R)
        out[pl.ds(start, R), half * H:(half + 1) * H] = value.astype(jnp.bfloat16)

    def both(e, k):
        return jnp.concatenate([g0[e, k, 0], g0[e, k, 1]], axis=0)

    put(0, b, 0, both(0, 0))
    put(0, b, 1, g1[0, 0])
    put(0, nb, 1, g1[0, 1])
    for k in range(1, A):
        put(k, b, 0, both(0, k))
    for k in near + ([2] if ring else []):
        for h in range(2):
            if (k, h) not in late:
                gz1[k, h].wait_recv()
        put(k, b, 1, g1[k, 0])
        put(k, nb, 1, g1[k, 1])
    for k in range(A):
        gy0[k].wait_recv()
        put(k, nb, 0, both(1, k))
    for k in range(A):
        y0[k].wait_send()
        gy0[k].wait_send()
    for pair in pairs:
        z0[pair].wait_send()
        z1[pair].wait_send()
        gz0[pair].wait_send()
        gz1[pair].wait_send()
    y1.wait_send()
    gy1.wait_send()


def coefficients(n_mem, img, pha, chosen, basis):
    rows, pixels = img.shape
    eigen = basis.shape[1]
    A, R, H = n_mem // 2, rows // n_mem, eigen // 2
    V = lambda *s: pltpu.VMEM(s, F32)
    D = lambda *s: pltpu.SemaphoreType.DMA(s)
    return pl.pallas_call(
        functools.partial(coeff_kernel, A, R, H),
        out_shape=jax.ShapeDtypeStruct((rows, eigen), jnp.bfloat16),
        in_specs=[pl.BlockSpec(memory_space=pltpu.VMEM)] * 4,
        out_specs=pl.BlockSpec(memory_space=pltpu.VMEM),
        scratch_shapes=[
            V(2, A, R, H), V(A, 2, R, H), V(A, R, H), V(A - 1, 2, R // 2, H), V(A - 1, 2, R // 2, H),
            V(A - 1, 2, R, H),
            V(R, H), V(R, H), V(2, A, 2, R // 2, H), V(A, 2, R, H),
            D(A), D(A), D(A - 1, 2), D(A - 1, 2), D(A - 1, 2), D(A - 1, 2),
            pltpu.SemaphoreType.DMA, pltpu.SemaphoreType.DMA,
            D(A - 1, 2), D(A - 1, 2), D(A), D(A),
            pltpu.SemaphoreType.DMA, pltpu.SemaphoreType.DMA, D(A - 1, 2), D(A - 1, 2),
        ],
        compiler_params=pltpu.CompilerParams(
            collective_id=0, has_side_effects=True, vmem_limit_bytes=48 * 1024 * 1024
        ),
    )(img, pha, chosen, basis)


def turn_to_row(col):
    return jnp.broadcast_to(col, (128, 128)).T[0:1]


def turn_to_col(row):
    return jnp.broadcast_to(row, (128, 128)).T[:, 0:1]


def update_kernel(
    M, X, NC, CW, RB, TR,
    coef, coef_t, prior, refs, out,
    p, stat, stat_r, scale, tot, mass, cr, cmr, xs, xms, xr, xmr,
    st_ss, st_rs, c_ss, c_rs, cm_ss, cm_rs, x_ss, x_rs, xm_ss, xm_rs,
):
    grp = lax.axis_index("grp")
    mem = lax.axis_index("mem")
    x, c = grp // 2, lax.rem(grp, 2)
    nc = 1 - c
    core = (x * 2 + nc, mem)
    rows = coef.shape[0]
    orient = refs.shape[1]
    S = rows // 128

    def xpeer(k):
        return (lax.rem(x + k, X) * 2 + c, mem)

    def mpeer(k):
        return (grp, lax.rem(mem + k, M))

    barrier = pltpu.get_barrier_semaphore()
    pl.semaphore_signal(barrier, inc=1, device_id=core, device_id_type=MESH)
    for k in range(1, X):
        pl.semaphore_signal(barrier, inc=1, device_id=xpeer(k), device_id_type=MESH)
    for k in range(1, M):
        pl.semaphore_signal(barrier, inc=1, device_id=mpeer(k), device_id_type=MESH)
    pl.semaphore_wait(barrier, X + M - 1)

    first_block = mem * (orient // OBLOCK)

    def score(t, carry):
        at = pl.ds(pl.multiple_of(t * TR, TR), TR)
        cf = coef[at, :]
        pr = prior[at, :]
        top = None
        for j in range(NC):
            s = jnp.dot(cf, refs[:, j * CW:(j + 1) * CW], preferred_element_type=F32)
            for i in range(CW // OBLOCK):
                inc = jnp.where(pr == first_block + (j * (CW // OBLOCK) + i), PRIOR_INCREMENT, 0.0).astype(F32)
                piece = s[:, i * OBLOCK:(i + 1) * OBLOCK] + inc
                p[at, j * CW + i * OBLOCK:j * CW + (i + 1) * OBLOCK] = piece
                high = jnp.max(piece, axis=1, keepdims=True)
                top = high if top is None else jnp.maximum(top, high)
        total = jnp.zeros((TR, 1), F32)
        for j in range(orient // OBLOCK):
            cols = slice(j * OBLOCK, (j + 1) * OBLOCK)
            e = jnp.exp(p[at, cols] - top)
            p[at, cols] = e
            total = total + jnp.sum(e, axis=1, keepdims=True)
        for i in range(TR // 128):
            stat[pl.ds(t * (TR // 128) + i, 1), :] = turn_to_row(top[i * 128:(i + 1) * 128])
            stat[pl.ds(S + t * (TR // 128) + i, 1), :] = turn_to_row(total[i * 128:(i + 1) * 128])
        return carry

    lax.fori_loop(0, rows // TR, score, 0)

    st = [None] + [
        remote(stat, stat_r.at[k - 1], st_ss.at[k - 1], st_rs.at[k - 1], mpeer(k)) for k in range(1, M)
    ]
    for k in range(1, M):
        st[k].start()
    for k in range(1, M):
        st[k].wait_recv()
    mine = stat[0:S, :]
    high = mine
    for k in range(1, M):
        high = jnp.maximum(high, stat_r[k - 1, 0:S, :])
    total = stat[S:2 * S, :] * jnp.exp(mine - high)
    for k in range(1, M):
        total = total + stat_r[k - 1, S:2 * S, :] * jnp.exp(stat_r[k - 1, 0:S, :] - high)
    factor = jnp.exp(mine - high) / total
    for i in range(S):
        scale[i * 128:(i + 1) * 128, :] = turn_to_col(factor[i:i + 1])

    def block_rows(k, cc):
        return pl.ds(pl.multiple_of((lax.rem(x + k, X) * 2 + cc) * RB, RB), RB)

    def c_copy(j, k):
        return remote(tot.at[j, block_rows(k, nc), :], cr.at[j, k], c_ss.at[j, k], c_rs.at[j, k], core)

    def cm_copy(j):
        return remote(mass.at[j], cmr.at[j], cm_ss.at[j], cm_rs.at[j], core)

    def x_copy(j, k):
        return remote(xs.at[j, k - 1], xr.at[j, k - 1], x_ss.at[j, k - 1], x_rs.at[j, k - 1], xpeer(k))

    def xm_copy(j, k):
        return remote(xms.at[j], xmr.at[j, k - 1], xm_ss.at[j, k - 1], xm_rs.at[j, k - 1], xpeer(k))

    def step(j, carry):
        @pl.when(j < NC)
        def _():
            cols = pl.ds(pl.multiple_of(j * CW, CW), CW)
            w = (p[:, cols] * scale[...]).astype(jnp.bfloat16)
            tot[j] = jnp.dot(coef_t[...], w, preferred_element_type=F32)
            mass[j] = jnp.broadcast_to(jnp.sum(w.astype(F32), axis=0, keepdims=True), (8, CW))
            for k in range(1, X):
                c_copy(j, k).start()
            cm_copy(j).start()
            c_copy(j, 0).start()

        @pl.when(j >= 1)
        def _():
            i = j - 1
            for k in range(1, X):
                c_copy(i, k).wait_recv()
                xs[i, k - 1] = tot[i, block_rows(k, c), :] + cr[i, k]
                x_copy(i, k).start()
            cm_copy(i).wait_recv()
            xms[i] = mass[i] + cmr[i]
            for k in range(1, X):
                xm_copy(i, k).start()

        return carry

    lax.fori_loop(0, NC + 1, step, 0)

    own_rows = block_rows(0, c)

    def finish(j, carry):
        cols = pl.ds(pl.multiple_of(j * CW, CW), CW)
        c_copy(j, 0).wait_recv()
        value = tot[j, own_rows, :] + cr[j, 0]
        m = xms[j]
        for k in range(1, X):
            x_copy(j, k).wait_recv()
            xm_copy(j, k).wait_recv()
            value = value + xr[j, k - 1]
            m = m + xmr[j, k - 1]
        out[:, cols] = (value + refs[own_rows, cols].astype(F32)) / (m[0:1] + 1.0)
        for k in range(X):
            c_copy(j, k).wait_send()
        cm_copy(j).wait_send()
        for k in range(1, X):
            x_copy(j, k).wait_send()
            xm_copy(j, k).wait_send()
        return carry

    lax.fori_loop(0, NC, finish, 0)
    for k in range(1, M):
        st[k].wait_send()


def update(n_grp, n_mem, coef, coef_t, prior, refs):
    rows, eigen = coef.shape
    orient = refs.shape[1]
    CW = min(512, orient)
    NC, RB, X, M = orient // CW, eigen // n_grp, n_grp // 2, n_mem
    S = rows // 128
    V = lambda *s: pltpu.VMEM(s, F32)
    D = lambda *s: pltpu.SemaphoreType.DMA(s)
    return pl.pallas_call(
        functools.partial(update_kernel, M, X, NC, CW, RB, 256),
        out_shape=jax.ShapeDtypeStruct((RB, orient), F32),
        in_specs=[pl.BlockSpec(memory_space=pltpu.VMEM)] * 4,
        out_specs=pl.BlockSpec(memory_space=pltpu.VMEM),
        scratch_shapes=[
            V(rows, orient), V(2 * S, 128), V(M - 1, 2 * S, 128), V(rows, 1),
            V(NC, eigen, CW), V(NC, 8, CW), V(NC, X, RB, CW), V(NC, 8, CW),
            V(NC, X - 1, RB, CW), V(NC, 8, CW), V(NC, X - 1, RB, CW), V(NC, X - 1, 8, CW),
            D(M - 1), D(M - 1), D(NC, X), D(NC, X), D(NC), D(NC),
            D(NC, X - 1), D(NC, X - 1), D(NC, X - 1), D(NC, X - 1),
        ],
        compiler_params=pltpu.CompilerParams(
            collective_id=1, has_side_effects=True, vmem_limit_bytes=67043328
        ),
    )(coef, coef_t, prior, refs)


def shards(n_grp, n_mem, images, phantom, inject_rows, prior_blocks, basis, refs):
    batches, particles, pixels = images.shape[1:]
    positions = jnp.arange(particles, dtype=jnp.int32)
    chosen = jnp.any(inject_rows[0][:, :, None] == positions[None, None, :], axis=1)
    chosen = chosen.astype(F32).reshape(batches * particles, 1)
    img = images.reshape(batches * particles, pixels)
    pha = jnp.broadcast_to(phantom, (16, pixels))
    coef = coefficients(n_mem, img, pha, chosen, basis)
    return update(n_grp, n_mem, coef, coef.T, prior_blocks.reshape(batches * particles, 1), refs)


def solution(mesh):
    placed = (
        P("grp", None, None, "mem"),
        P("grp", "mem"),
        P("grp", None, None),
        P("grp", None, None),
        P("mem", None),
        P(None, "mem"),
    )
    return jax.shard_map(
        functools.partial(shards, mesh.shape["grp"], mesh.shape["mem"]),
        mesh=mesh, in_specs=placed, out_specs=P("grp", "mem"), check_vma=False,
    )
```
